32 devices in a mesh: row: 16 (over z, y, core), col: 2 (over x).
Axes of the slice: x: 2, y: 2, z: 4, core: 2. Of those that a mesh axis runs over, the one named last changes fastest.
Arguments:
- vectors: float32 [1024, 32768], P(('row', 'col')), may hold values from -6 to 6
- reflectors: float32 [6, 128, 32768], P(None, 'col', 'row')
- factors: float32 [6, 128, 128], replicated, as said below
Outputs:
- transformed: float32 [1024, 32768], P('col', 'row')
The draws below stay inside these ranges and needn't reach their ends.
Inputs may be any that keep to these rules, and one draw needn't show every extreme that they name: factors[k] is upper triangular, and its inverse equals the strict upper part of reflectors[k] reflectors[k]^T plus half of that product's diagonal, so each panel is orthogonal.
All inputs are finite; a program needn't handle non-finite values.
Results may differ from the reference program's by a relative error of at most 0.0001.
Values sent between devices are 32-bit elements; how exact they have to be, the bound alone decides.
A program may use at most 128 MiB of HBM per device.

```python
import jax
import jax.numpy as jnp
from jax import lax

N = 32768
BLOCK = 128
PANELS = 6
EIGVECS = 1024


def invert_upper(matrix):
    identity = jnp.eye(matrix.shape[0], dtype=jnp.float32)
    return jax.scipy.linalg.solve_triangular(matrix, identity, lower=False)


def reflector_pair(key):
    random_part = jax.random.normal(jax.random.fold_in(key, 11), (PANELS, BLOCK, N), jnp.float32) / jnp.sqrt(jnp.float32(N))
    mixing = jnp.eye(BLOCK, dtype=jnp.float32) + 0.35 / jnp.sqrt(jnp.float32(BLOCK)) * jax.random.normal(jax.random.fold_in(key, 12), (PANELS, BLOCK, BLOCK), jnp.float32)
    reflect = jnp.einsum('pij,pjn->pin', mixing, random_part, precision=lax.Precision.HIGHEST)
    gram_matrix = jnp.einsum('pin,pjn->pij', reflect, reflect, precision=lax.Precision.HIGHEST)
    diagonal_half = 0.5 * jnp.einsum('pii->pi', gram_matrix)
    inverse = jnp.triu(gram_matrix, 1) + jax.vmap(jnp.diag)(diagonal_half)
    triangle = jax.vmap(invert_upper)(inverse)
    return (reflect, triangle)


def draw_reflectors(key, part):
    return reflector_pair(jax.random.fold_in(key, 7))[0]


def draw_factors(key, part):
    return reflector_pair(jax.random.fold_in(key, 7))[1]


def levels(own_key, extent, cuts, low, largest):
    gain = 1.0
    for position, shards_of in cuts:
        steps = jax.random.uniform(jax.random.fold_in(jax.random.fold_in(own_key, 6), position), (shards_of,), jnp.float32, low / len(cuts), largest / len(cuts))
        gain = gain * jnp.repeat(jnp.exp(steps), extent[position] // shards_of).reshape((-1,) + (1,) * (len(extent) - 1 - position))
    return gain


def gaussian(rng, extent, width, limit, pieces=(), kind=jnp.bfloat16):
    result = jax.random.normal(rng, extent, jnp.float32) * width
    if len(pieces) > 0:
        result = levels(rng, extent, pieces, -0.22, 0.18) * result
    return jnp.clip(result, min=-limit, max=limit).astype(kind)


def setup_inputs(seed: int = 0) -> dict:
    keys = jax.random.split(jax.random.key(seed), 4)
    return {
        "vectors": gaussian(keys[0], (EIGVECS, N), 1.0, 6.0, ((0, 32),), jnp.float32),
        "reflectors": draw_reflectors(jax.random.fold_in(keys[3], 71), 0),
        "factors": draw_factors(jax.random.fold_in(keys[3], 71), 0),
    }


def reference(vectors, reflectors, factors):
    current = vectors
    for panel in range(PANELS - 1, -1, -1):
        stacked = reflectors[panel]
        projection = lax.dot_general(current.astype(jnp.float32), stacked.astype(jnp.float32), (((1,), (1,)), ((), ())), precision=lax.Precision.HIGHEST, preferred_element_type=jnp.float32)
        update = jnp.dot(projection.astype(jnp.float32), factors[panel].T.astype(jnp.float32), precision=lax.Precision.HIGHEST, preferred_element_type=jnp.float32)
        current = current - jnp.dot(update.astype(jnp.float32), stacked.astype(jnp.float32), precision=lax.Precision.HIGHEST, preferred_element_type=jnp.float32)
    return current
```

```python
import functools

import jax
import jax.numpy as jnp
from jax import lax
from jax.experimental import pallas as pl
from jax.experimental.pallas import tpu as pltpu
from jax.sharding import PartitionSpec as P

MESH = pl.DeviceIdType.MESH
HIGHEST = lax.Precision.HIGHEST
SUB = 8


def nt(left, right, precision=None):
    return lax.dot_general(
        left,
        right,
        (((1,), (1,)), ((), ())),
        precision=precision,
        preferred_element_type=jnp.float32,
    )


def nn(left, right, precision=None):
    return jnp.dot(left, right, precision=precision, preferred_element_type=jnp.float32)


def split(value):
    top = value.astype(jnp.bfloat16)
    return top, (value - top.astype(jnp.float32)).astype(jnp.bfloat16)


def doubled(value, width):
    columns = value.shape[1]
    pieces = []
    for part in split(value):
        twice = []
        for start in range(0, columns, width):
            piece = part[:, start : start + width]
            twice += [piece, piece]
        pieces.append(jnp.concatenate(twice, axis=1))
    return jnp.concatenate(pieces, axis=0)


def bits_of(count):
    return count.bit_length() - 1


def bit(value, stride):
    return (value // stride) % 2


def mirrored(value, bits):
    found = 0
    for i in range(bits):
        found = found + bit(value, 1 << i) * (1 << (bits - 1 - i))
    return found


class Chain:
    def __init__(self, steps):
        self.steps = list(steps)
        self.open = None

    def tick(self):
        if self.open is not None:
            self.open()
            self.open = None
        if self.steps:
            start, end = self.steps.pop(0)
            start()
            self.open = end


def tick(*chains):
    for chain in chains:
        if chain.open is not None:
            chain.open()
            chain.open = None
    for chain in chains:
        chain.tick()


def kernel(
    row_count, col_count, vectors, reflectors, factors, out,
    stage, here, held, both, mixed, projection, landing, wide, solved, weights,
    system, pairs, partial, gram_landing, gram,
    row_sems, local_sems, gather_sems, far_sems, sum_sems, cross_sems, wide_sems,
    gram_sems, out_sems,
):
    row = lax.axis_index("row")
    col = lax.axis_index("col")
    chunks = stage.shape[0]
    local = chunks * SUB
    length = held.shape[1]
    count, part, _ = reflectors.shape
    width = part * col_count
    group = row_count // col_count
    row_bits, col_bits, group_bits = bits_of(row_count), bits_of(col_count), bits_of(group)
    rows = row_count * SUB
    high, low = row // group, row % group
    my_place = mirrored(low, group_bits)

    barrier = pltpu.get_barrier_semaphore()
    for step in range(1, row_count):
        pl.semaphore_signal(
            barrier, inc=1, device_id={"row": lax.rem(row + step, row_count)}, device_id_type=MESH
        )
    for step in range(1, col_count):
        pl.semaphore_signal(
            barrier, inc=1, device_id={"col": lax.rem(col + step, col_count)}, device_id_type=MESH
        )
    pairing = [
        (dh, dc) for dh in range(1, col_count) for dc in range(1, col_count)
    ]
    for dh, dc in pairing:
        pl.semaphore_signal(
            barrier,
            inc=1,
            device_id={
                "row": lax.rem(high + dh, col_count) * group + low,
                "col": lax.rem(col + dc, col_count),
            },
            device_id_type=MESH,
        )
    pl.semaphore_wait(barrier, row_count + col_count - 2 + len(pairing))

    def remote(source, target, sems, number, device, arrival=None):
        return pltpu.make_async_remote_copy(
            src_ref=source,
            dst_ref=target,
            send_sem=sems.at[0, number],
            recv_sem=sems.at[1, number if arrival is None else arrival],
            device_id=device,
            device_id_type=MESH,
        )

    order = list(range(count - 1, -1, -1))
    gathers = {}
    for panel in order:
        place = held.at[pl.ds(pl.multiple_of(panel * width + col * part, SUB), part)]
        gathers[panel] = []
        for step in range(1, col_count):
            item = remote(
                reflectors.at[panel], place, gather_sems, (step - 1) * count + panel,
                {"col": lax.rem(col + step, col_count)},
            )
            item.start()
            gathers[panel].append(item)
    for panel in order:
        place = held.at[pl.ds(pl.multiple_of(panel * width + col * part, SUB), part)]
        item = pltpu.make_async_copy(reflectors.at[panel], place, local_sems.at[panel])
        item.start()
        gathers[panel].append(item)

    middle = row_count // 2
    ranked = sorted(range(1, row_count), key=lambda step: (abs(step - middle), step))
    steps = []
    while ranked:
        steps.append(ranked.pop(0))
        if ranked:
            steps.append(ranked.pop())
    arrivals = {}

    def send_rows(chunk):
        place = stage.at[
            chunk, my_place,
            pl.ds(pl.multiple_of(mirrored(high, col_bits) * SUB, SUB), SUB),
        ]
        taken = pl.ds(chunk * SUB, SUB)
        items = []
        for step in steps:
            other = lax.rem(row + step, row_count)
            item = remote(
                vectors.at[taken, pl.ds(pl.multiple_of(other * length, 128), length)],
                place, row_sems, chunk * row_count + step, {"row": other},
            )
            item.start()
            items.append(item)
        item = pltpu.make_async_copy(
            vectors.at[taken, pl.ds(pl.multiple_of(row * length, 128), length)],
            place, local_sems.at[count + chunk],
        )
        item.start()
        items.append(item)
        arrivals[chunk] = items

    for chunk in range(chunks):
        send_rows(chunk)

    def take_rows(chunk):
        for item in arrivals[chunk]:
            item.wait()
        own = pl.ds(pl.multiple_of(mirrored(col, col_bits) * SUB, SUB), SUB)
        mine = pl.ds(pl.multiple_of(col * SUB, SUB), SUB)
        size = col_count * SUB

        def body(i, carry):
            top, low_part = split(stage[chunk, i])
            at = pl.multiple_of(i * size, size)
            mixed[chunk, pl.ds(at, size), :] = top
            mixed[chunk, pl.ds(pl.multiple_of(rows + at, size), size), :] = low_part
            here[chunk, i, mine, :] = stage[chunk, i, own, :]
            return carry

        lax.fori_loop(0, group, body, 0)

    def take_panel(panel):
        for item in gathers[panel]:
            item.wait()

        def body(i, carry):
            at = pl.multiple_of(panel * width + i * 32, 32)
            top, low_part = split(held[pl.ds(at, 32), :])
            to = pl.multiple_of(2 * panel * width + i * 32, 32)
            both[pl.ds(to, 32), :] = top
            both[pl.ds(pl.multiple_of(to + width, 32), 32), :] = low_part
            return carry

        lax.fori_loop(0, width // 32, body, 0)

    def panel_rows(panel):
        return pl.ds(pl.multiple_of(2 * panel * width, 2 * width), 2 * width)

    def quadrants(value, above, left):
        value = value[:above] + value[above:]
        return value[:, :left] + value[:, left:]

    bases = {}
    base = 0
    for panel in range(count - 2, -1, -1):
        bases[panel] = base
        base += (count - 1 - panel) * width

    def inner(panel):
        def body(i, carry):
            value = nt(both[panel_rows(panel + 1 + i), :], both[panel_rows(panel), :])
            to = pl.multiple_of(bases[panel] + i * width, width)
            partial[pl.ds(to, width), :] = quadrants(value, width, width)
            return carry

        if panel < count - 1:
            lax.fori_loop(0, count - 1 - panel, body, 0)

    def project(chunk, first, last):
        def body(i, carry):
            value = nt(mixed[chunk], both[panel_rows(first + i), :])
            to = pl.ds(pl.multiple_of((first + i) * width, width), width)
            projection[chunk, :, to] = quadrants(value, rows, width)
            return carry

        lax.fori_loop(0, last - first, body, 0)

    def halving(source, target, sems, number):
        total = source.shape[0]
        state = {"now": source}
        steps = []
        for stage_number in range(row_bits):
            stride = 1 << stage_number
            half = total >> (stage_number + 1)
            start = total - (total >> stage_number)

            def begin(stride=stride, half=half, start=start, stage_number=stage_number):
                away = pl.ds(pl.multiple_of((1 - bit(row, stride)) * half, SUB), half)
                place = target.at[pl.ds(start, half)]
                item = remote(
                    state["now"].at[away], place, sems, number + stage_number,
                    {"row": row + stride * (1 - 2 * bit(row, stride))},
                )
                item.start()
                state["item"], state["place"] = item, place

            def end(stride=stride, half=half):
                state["item"].wait()
                keep = pl.ds(pl.multiple_of(bit(row, stride) * half, SUB), half)
                place = state["place"]
                place[...] = place[...] + state["now"][keep, :]
                state["now"] = place

            steps.append((begin, end))
        return Chain(steps), state

    def doubling(strides, target, sems, number, position, size):
        state = {"position": position, "size": size}
        steps = []
        for stage_number, stride in enumerate(strides):
            def begin(stride=stride, stage_number=stage_number):
                where = target.at[pl.ds(state["position"], state["size"])]
                item = remote(
                    where, where, sems, number + stage_number,
                    {"row": row + stride * (1 - 2 * bit(row, stride))},
                )
                item.start()
                state["item"] = item

            def end(stride=stride):
                state["item"].wait()
                state["position"] = state["position"] - bit(row, stride) * state["size"]
                state["size"] = state["size"] * 2

            steps.append((begin, end))
        return steps

    def cross(chunk):
        rows_of = pl.ds(pl.multiple_of(col * SUB, SUB), SUB)
        items = []
        base = chunk * col_count

        def begin():
            place = wide.at[chunk, my_place, rows_of]
            for step in range(col_count):
                other = lax.rem(high + step, col_count)
                item = remote(
                    solved.at[chunk], place, cross_sems, base + step,
                    {"row": other * group + low, "col": high}, base + col,
                )
                items.append(item)
                if step:
                    item.start()

            @pl.when(col != high)
            def _():
                items[0].start()

            @pl.when(col == high)
            def _():
                wide[chunk, my_place, rows_of, :] = solved[chunk]

        def end():
            for step in range(1, col_count):
                items[step].wait_send()

            @pl.when(col != high)
            def _():
                items[0].wait_send()

            for other in range(col_count):
                item = remote(
                    solved.at[chunk],
                    wide.at[chunk, my_place, pl.ds(other * SUB, SUB)],
                    cross_sems, base, {"row": row, "col": col}, base + other,
                )

                @pl.when((col != high) | (col != other))
                def _():
                    item.wait_recv()

        return begin, end

    def spread(chunk):
        strides = [group >> (i + 1) for i in range(group_bits)]
        return Chain(
            [cross(chunk)]
            + doubling(strides, wide.at[chunk], wide_sems, chunk * max(group_bits, 1), my_place, 1)
        )

    far = {}

    def send_far(chunk):
        items = []
        for step in range(1, col_count):
            other = lax.rem(col + step, col_count)
            source = pl.ds(pl.multiple_of(mirrored(other, col_bits) * SUB, SUB), SUB)
            target = pl.ds(pl.multiple_of(col * SUB, SUB), SUB)
            item = remote(
                stage.at[chunk, :, source], here.at[chunk, :, target],
                far_sems, chunk * col_count + step, {"col": other},
            )
            item.start()
            items.append(item)
        far[chunk] = items

    def build():
        system[...] = jnp.zeros_like(system)
        for panel in range(count - 1, -1, -1):
            at = pl.ds(panel * width, width)
            system[at, at] = factors[panel].T
            if panel < count - 1:
                below = pl.ds((panel + 1) * width, (count - 1 - panel) * width)
                value = nn(
                    system[below, below], gram[pl.ds(bases[panel], below.size), :], HIGHEST
                )
                system[below, at] = -nt(value, factors[panel], HIGHEST)
        for panel in range(count):
            top, low_part = split(system[pl.ds(panel * width, width), :])
            pairs[pl.ds(2 * panel * width, width), :] = top
            pairs[pl.ds((2 * panel + 1) * width, width), :] = low_part

    def solve(states, numbers):
        value = jnp.concatenate([states[number]["now"][...] for number in numbers], axis=0)
        size = value.shape[0]
        value = nn(doubled(value, width), pairs[...])
        value = value[:size] + value[size:]
        for i, number in enumerate(numbers):
            solved[number] = value[i * SUB : (i + 1) * SUB]

    outs = []
    tile = 512 if length % 512 == 0 else length

    def update(chunk):
        for item in far[chunk]:
            item.wait()
        weights[...] = doubled(wide[chunk].reshape(rows, count * width), width)

        def body(i, carry):
            at = pl.ds(pl.multiple_of(i * tile, tile), tile)
            value = nn(weights[...], both[:, at])
            value = (value[:rows] + value[rows:]).reshape(group, col_count * SUB, tile)
            here[chunk, :, :, at] = here[chunk, :, :, at] - value
            return carry

        lax.fori_loop(0, length // tile, body, 0)
        for place in range(group):
            for other in range(col_count):
                slot = mirrored(place, group_bits) * col_count + other
                item = pltpu.make_async_copy(
                    here.at[chunk, place, pl.ds(other * SUB, SUB)],
                    out.at[pl.ds(slot * local + chunk * SUB, SUB)],
                    out_sems.at[chunk * row_count + place * col_count + other],
                )
                item.start()
                outs.append(item)

    due = [((chunk + 1) / chunks, 1, chunk) for chunk in range(chunks - 1)]
    due += [(0.78 * (i + 1) / count, 0, panel) for i, panel in enumerate(order)]
    ready_rows, done = [], {}
    lowest = count
    for _, kind, number in sorted(due):
        if kind == 0:
            take_panel(number)
            inner(number)
            lowest = number
        else:
            take_rows(number)
            ready_rows.append(number)
            done[number] = count
        last = number == 0 and kind == 0
        for chunk in ready_rows:
            if done[chunk] - lowest >= 2 or (lowest == 0 and done[chunk] > 0):
                project(chunk, lowest, done[chunk])
                done[chunk] = lowest
    early = list(range(chunks - 1))
    late = chunks - 1
    for chunk in early:
        send_far(chunk)
    sums = {}
    states = {}
    for chunk in range(chunks):
        sums[chunk], states[chunk] = halving(
            projection.at[chunk], landing.at[chunk], sum_sems, chunk * row_bits
        )
    gram_rows = gram.shape[0]
    used = bases[0] + (count - 1) * width
    if used < gram_rows:
        partial[pl.ds(used, gram_rows - used), :] = jnp.zeros((gram_rows - used, width), jnp.float32)
    gram_chain, gram_state = halving(partial, gram_landing, gram_sems, 0)
    first = [sums[chunk] for chunk in early]
    tick(gram_chain, *first)
    for number in range(row_bits):
        tick(gram_chain, *first)
    piece = gram_rows // row_count
    place = mirrored(row, row_bits) * piece
    gram[pl.ds(pl.multiple_of(place, SUB), piece), :] = gram_state["now"][...]
    strides = [1 << i for i in range(row_bits - 1, -1, -1)]
    gram_chain = Chain(
        doubling(strides, gram, gram_sems, row_bits, pl.multiple_of(place, SUB), piece)
    )
    tick(gram_chain)
    for number in range(row_bits - 2):
        tick(gram_chain)
    take_rows(late)
    send_far(late)
    project(late, 0, count)
    tick(gram_chain, sums[late])
    tick(gram_chain)
    build()
    solve(states, early)
    spreads = {chunk: spread(chunk) for chunk in range(chunks)}
    first = [spreads[chunk] for chunk in early]
    for number in range(row_bits):
        tick(sums[late], *first)
    solve(states, [late])
    tick(spreads[late], *first)
    for number in range(max(group_bits - row_bits, 0)):
        tick(*first)
    for chunk in early[:-1]:
        update(chunk)
    tick(spreads[late])
    if early:
        update(early[-1])
    for number in range(group_bits):
        tick(spreads[late])
    update(late)
    for item in outs:
        item.wait()


def on_device(vectors, reflectors, factors):
    local, total_length = vectors.shape
    row_count = lax.axis_size("row")
    col_count = lax.axis_size("col")
    length = total_length // row_count
    count, part, _ = reflectors.shape
    width = part * col_count
    every = count * width
    chunks = local // SUB
    group = row_count // col_count
    row_bits, group_bits = bits_of(row_count), bits_of(group)
    rows = row_count * SUB
    unit = SUB * row_count
    gram_rows = -(-(count * (count - 1) // 2 * width) // unit) * unit
    anywhere = pl.BlockSpec(memory_space=pl.ANY)
    vmem = pl.BlockSpec(memory_space=pltpu.VMEM)
    dma = pltpu.SemaphoreType.DMA
    single, half = jnp.float32, jnp.bfloat16
    return pl.pallas_call(
        functools.partial(kernel, row_count, col_count),
        name="exchange",
        out_shape=jax.ShapeDtypeStruct((local * row_count, length), single),
        in_specs=[anywhere, anywhere, vmem],
        out_specs=anywhere,
        scratch_shapes=[
            pltpu.VMEM((chunks, group, col_count * SUB, length), single),
            pltpu.VMEM((chunks, group, col_count * SUB, length), single),
            pltpu.VMEM((every, length), single),
            pltpu.VMEM((2 * every, length), half),
            pltpu.VMEM((chunks, 2 * rows, length), half),
            pltpu.VMEM((chunks, rows, every), single),
            pltpu.VMEM((chunks, rows, every), single),
            pltpu.VMEM((chunks, group, col_count * SUB, every), single),
            pltpu.VMEM((chunks, SUB, every), single),
            pltpu.VMEM((2 * rows, 2 * every), half),
            pltpu.VMEM((every, every), single),
            pltpu.VMEM((2 * every, every), half),
            pltpu.VMEM((gram_rows, width), single),
            pltpu.VMEM((gram_rows, width), single),
            pltpu.VMEM((gram_rows, width), single),
            dma((2, chunks * row_count)),
            dma((count + chunks,)),
            dma((2, (col_count - 1) * count)),
            dma((2, chunks * col_count)),
            dma((2, chunks * row_bits)),
            dma((2, chunks * col_count)),
            dma((2, chunks * max(group_bits, 1))),
            dma((2, 2 * row_bits)),
            dma((chunks * row_count,)),
        ],
        compiler_params=pltpu.CompilerParams(
            collective_id=0, has_side_effects=True, vmem_limit_bytes=60 * 1024 * 1024
        ),
    )(vectors, reflectors, factors)


def solution(mesh):
    return jax.shard_map(
        on_device,
        mesh=mesh,
        in_specs=(P(("row", "col"), None), P(None, "col", "row"), P()),
        out_specs=P("col", "row"),
        check_vma=False,
    )
```

```python
import functools

import jax
import jax.numpy as jnp
from jax import lax
from jax.experimental import pallas as pl
from jax.experimental.pallas import tpu as pltpu
from jax.sharding import PartitionSpec as P

MESH = pl.DeviceIdType.MESH
HIGHEST = lax.Precision.HIGHEST
SUB = 8
WIDER = -5
GAP0 = 0.025
GAP = 0.1
AFTER = 0


def nt(left, right, precision=None):
    return lax.dot_general(
        left,
        right,
        (((1,), (1,)), ((), ())),
        precision=precision,
        preferred_element_type=jnp.float32,
    )


def nn(left, right, precision=None):
    return jnp.dot(left, right, precision=precision, preferred_element_type=jnp.float32)


def split(value):
    top = value.astype(jnp.bfloat16)
    return top, (value - top.astype(jnp.float32)).astype(jnp.bfloat16)


def doubled(value, width):
    columns = value.shape[1]
    pieces = []
    for part in split(value):
        twice = []
        for start in range(0, columns, width):
            piece = part[:, start : start + width]
            twice += [piece, piece]
        pieces.append(jnp.concatenate(twice, axis=1))
    return jnp.concatenate(pieces, axis=0)


def bits_of(count):
    return count.bit_length() - 1


def bit(value, stride):
    return (value // stride) % 2


def mirrored(value, bits):
    found = 0
    for i in range(bits):
        found = found + bit(value, 1 << i) * (1 << (bits - 1 - i))
    return found


def batches(count):
    found = [list(range(count - 2, 1, -1)), [1], [0]]
    return [[panel for panel in panels if panel < count - 1] for panels in found if panels]


def padded(size, row_count):
    unit = SUB * row_count
    return -(-size // unit) * unit


class Chain:
    def __init__(self, steps):
        self.steps = list(steps)
        self.open = None
        self.due = 0.0
        self.made = 0

    def tick_at(self, time):
        if time >= self.due:
            self.tick()
            self.due = time + (GAP0 if self.made == 0 else GAP)
            self.made += 1

    def tick(self):
        if self.open is not None:
            self.open()
            self.open = None
        if self.steps:
            start, end = self.steps.pop(0)
            start()
            self.open = end


def tick(*chains):
    for chain in chains:
        chain.tick()


def busy(*chains):
    return any(chain.open is not None or chain.steps for chain in chains)


def kernel(
    row_count, col_count, vectors, reflectors, factors, out,
    stage, here, held, both, mixed, projection, landing, wide, solved, weights,
    system, pairs, partial, gram_landing, gram,
    row_sems, local_sems, gather_sems, far_sems, sum_sems, cross_sems, wide_sems,
    gram_sems, out_sems,
):
    row = lax.axis_index("row")
    col = lax.axis_index("col")
    chunks = stage.shape[0]
    local = chunks * SUB
    length = held.shape[1]
    count, part, _ = reflectors.shape
    width = part * col_count
    group = row_count // col_count
    row_bits, col_bits, group_bits = bits_of(row_count), bits_of(col_count), bits_of(group)
    rows = row_count * SUB
    high, low = row // group, row % group
    my_place = mirrored(low, group_bits)

    barrier = pltpu.get_barrier_semaphore()
    for step in range(1, row_count):
        pl.semaphore_signal(
            barrier, inc=1, device_id={"row": lax.rem(row + step, row_count)}, device_id_type=MESH
        )
    for step in range(1, col_count):
        pl.semaphore_signal(
            barrier, inc=1, device_id={"col": lax.rem(col + step, col_count)}, device_id_type=MESH
        )
    pairing = [
        (dh, dc) for dh in range(1, col_count) for dc in range(1, col_count)
    ]
    for dh, dc in pairing:
        pl.semaphore_signal(
            barrier,
            inc=1,
            device_id={
                "row": lax.rem(high + dh, col_count) * group + low,
                "col": lax.rem(col + dc, col_count),
            },
            device_id_type=MESH,
        )
    pl.semaphore_wait(barrier, row_count + col_count - 2 + len(pairing))

    def remote(source, target, sems, number, device, arrival=None):
        return pltpu.make_async_remote_copy(
            src_ref=source,
            dst_ref=target,
            send_sem=sems.at[0, number],
            recv_sem=sems.at[1, number if arrival is None else arrival],
            device_id=device,
            device_id_type=MESH,
        )

    order = list(range(count - 1, -1, -1))
    gathers = {}
    for panel in order:
        place = held.at[pl.ds(pl.multiple_of(panel * width + col * part, SUB), part)]
        gathers[panel] = []
        for step in range(1, col_count):
            item = remote(
                reflectors.at[panel], place, gather_sems, (step - 1) * count + panel,
                {"col": lax.rem(col + step, col_count)},
            )
            item.start()
            gathers[panel].append(item)
    for panel in order:
        place = held.at[pl.ds(pl.multiple_of(panel * width + col * part, SUB), part)]
        item = pltpu.make_async_copy(reflectors.at[panel], place, local_sems.at[panel])
        item.start()
        gathers[panel].append(item)

    middle = row_count // 2
    ranked = sorted(range(1, row_count), key=lambda step: (abs(step - middle), step))
    steps = []
    while ranked:
        steps.append(ranked.pop(0))
        if ranked:
            steps.append(ranked.pop())
    place = stage.at[
        :, my_place, pl.ds(pl.multiple_of(mirrored(high, col_bits) * SUB, SUB), SUB)
    ]
    sends = []
    for chunk in range(chunks):
        for step in steps:
            other = lax.rem(row + step, row_count)
            item = remote(
                vectors.at[
                    pl.ds(chunk * SUB, SUB), pl.ds(pl.multiple_of(other * length, 128), length)
                ],
                place.at[chunk], row_sems, chunk * row_count + step, {"row": other},
            )
            sends.append(item)
    own_rows = []
    for chunk in range(chunks):
        item = pltpu.make_async_copy(
            vectors.at[
                pl.ds(chunk * SUB, SUB), pl.ds(pl.multiple_of(row * length, 128), length)
            ],
            place.at[chunk], local_sems.at[count + chunk],
        )
        item.start()
        own_rows.append(item)
    window = len(steps) + WIDER
    for item in sends[:window]:
        item.start()

    def arrive(number):
        sends[number].wait()
        if number + window < len(sends):
            sends[number + window].start()

    def take_rows(chunk):
        own_rows[chunk].wait()
        own = pl.ds(pl.multiple_of(mirrored(col, col_bits) * SUB, SUB), SUB)
        mine = pl.ds(pl.multiple_of(col * SUB, SUB), SUB)
        size = col_count * SUB

        def body(i, carry):
            top, low_part = split(stage[chunk, i])
            at = pl.multiple_of(i * size, size)
            mixed[chunk, pl.ds(at, size), :] = top
            mixed[chunk, pl.ds(pl.multiple_of(rows + at, size), size), :] = low_part
            here[chunk, i, mine, :] = stage[chunk, i, own, :]
            return carry

        lax.fori_loop(0, group, body, 0)

    def take_panel(panel):
        for item in gathers[panel]:
            item.wait()

        def body(i, carry):
            at = pl.multiple_of(panel * width + i * 32, 32)
            top, low_part = split(held[pl.ds(at, 32), :])
            to = pl.multiple_of(2 * panel * width + i * 32, 32)
            both[pl.ds(to, 32), :] = top
            both[pl.ds(pl.multiple_of(to + width, 32), 32), :] = low_part
            return carry

        lax.fori_loop(0, width // 32, body, 0)

    def panel_rows(panel):
        return pl.ds(pl.multiple_of(2 * panel * width, 2 * width), 2 * width)

    def quadrants(value, above, left):
        value = value[:above] + value[above:]
        return value[:, :left] + value[:, left:]

    bases, bounds = {}, []
    base = 0
    for panels in batches(count):
        first = base
        for panel in panels:
            bases[panel] = base
            base += (count - 1 - panel) * width
        used = base
        base = first + padded(used - first, row_count)
        if used < base:
            partial[pl.ds(used, base - used), :] = jnp.zeros((base - used, width), jnp.float32)
        bounds.append((first, base - first))

    def inner(panel):
        def body(i, carry):
            value = nt(both[panel_rows(panel + 1 + i), :], both[panel_rows(panel), :])
            to = pl.multiple_of(bases[panel] + i * width, width)
            partial[pl.ds(to, width), :] = quadrants(value, width, width)
            return carry

        if panel < count - 1:
            lax.fori_loop(0, count - 1 - panel, body, 0)

    def project(chunk, first, last):
        def body(i, carry):
            value = nt(mixed[chunk], both[panel_rows(first + i), :])
            to = pl.ds(pl.multiple_of((first + i) * width, width), width)
            projection[chunk, :, to] = quadrants(value, rows, width)
            return carry

        lax.fori_loop(0, last - first, body, 0)

    def halving(source, target, sems, number):
        total = source.shape[0]
        state = {"now": source}
        steps = []
        for stage_number in range(row_bits):
            stride = 1 << stage_number
            half = total >> (stage_number + 1)
            start = total - (total >> stage_number)

            def begin(stride=stride, half=half, start=start, stage_number=stage_number):
                away = pl.ds(pl.multiple_of((1 - bit(row, stride)) * half, SUB), half)
                place = target.at[pl.ds(start, half)]
                item = remote(
                    state["now"].at[away], place, sems, number + stage_number,
                    {"row": row + stride * (1 - 2 * bit(row, stride))},
                )
                item.start()
                state["item"], state["place"] = item, place

            def end(stride=stride, half=half):
                state["item"].wait()
                keep = pl.ds(pl.multiple_of(bit(row, stride) * half, SUB), half)
                place = state["place"]
                place[...] = place[...] + state["now"][keep, :]
                state["now"] = place

            steps.append((begin, end))
        return Chain(steps), state

    def doubling(strides, target, sems, number, position, size):
        state = {"position": position, "size": size}
        steps = []
        for stage_number, stride in enumerate(strides):
            def begin(stride=stride, stage_number=stage_number):
                where = target.at[pl.ds(state["position"], state["size"])]
                item = remote(
                    where, where, sems, number + stage_number,
                    {"row": row + stride * (1 - 2 * bit(row, stride))},
                )
                item.start()
                state["item"] = item

            def end(stride=stride):
                state["item"].wait()
                state["position"] = state["position"] - bit(row, stride) * state["size"]
                state["size"] = state["size"] * 2

            steps.append((begin, end))
        return steps

    def cross(chunk):
        rows_of = pl.ds(pl.multiple_of(col * SUB, SUB), SUB)
        items = []
        base = chunk * col_count

        def begin():
            place = wide.at[chunk, my_place, rows_of]
            for step in range(col_count):
                other = lax.rem(high + step, col_count)
                item = remote(
                    solved.at[chunk], place, cross_sems, base + step,
                    {"row": other * group + low, "col": high}, base + col,
                )
                items.append(item)
                if step:
                    item.start()

            @pl.when(col != high)
            def _():
                items[0].start()

            @pl.when(col == high)
            def _():
                wide[chunk, my_place, rows_of, :] = solved[chunk]

        def end():
            for step in range(1, col_count):
                items[step].wait_send()

            @pl.when(col != high)
            def _():
                items[0].wait_send()

            for other in range(col_count):
                item = remote(
                    solved.at[chunk],
                    wide.at[chunk, my_place, pl.ds(other * SUB, SUB)],
                    cross_sems, base, {"row": row, "col": col}, base + other,
                )

                @pl.when((col != high) | (col != other))
                def _():
                    item.wait_recv()

        return begin, end

    def spread(chunk):
        strides = [group >> (i + 1) for i in range(group_bits)]
        return Chain(
            [cross(chunk)]
            + doubling(strides, wide.at[chunk], wide_sems, chunk * max(group_bits, 1), my_place, 1)
        )

    far = {}

    def send_far(chunk):
        items = []
        for step in range(1, col_count):
            other = lax.rem(col + step, col_count)
            source = pl.ds(pl.multiple_of(mirrored(other, col_bits) * SUB, SUB), SUB)
            target = pl.ds(pl.multiple_of(col * SUB, SUB), SUB)
            item = remote(
                stage.at[chunk, :, source], here.at[chunk, :, target],
                far_sems, chunk * col_count + step, {"col": other},
            )
            item.start()
            items.append(item)
        far[chunk] = items

    def build(panel):
        at = pl.ds(panel * width, width)
        system[at, at] = factors[panel].T
        if panel < count - 1:
            below = pl.ds((panel + 1) * width, (count - 1 - panel) * width)
            value = nn(system[below, below], gram[pl.ds(bases[panel], below.size), :], HIGHEST)
            system[below, at] = -nt(value, factors[panel], HIGHEST)

    def finish():
        for panel in range(count):
            top, low_part = split(system[pl.ds(panel * width, width), :])
            pairs[pl.ds(2 * panel * width, width), :] = top
            pairs[pl.ds((2 * panel + 1) * width, width), :] = low_part

    outs = []
    tile = 512 if length % 512 == 0 else length

    def update(chunk):
        for item in far[chunk]:
            item.wait()
        value = nn(doubled(wide[chunk].reshape(rows, count * width), width), pairs[...])
        weights[...] = doubled(value[:rows] + value[rows:], width)

        def body(i, carry):
            at = pl.ds(pl.multiple_of(i * tile, tile), tile)
            value = nn(weights[...], both[:, at])
            value = (value[:rows] + value[rows:]).reshape(group, col_count * SUB, tile)
            here[chunk, :, :, at] = here[chunk, :, :, at] - value
            return carry

        lax.fori_loop(0, length // tile, body, 0)
        for place in range(group):
            for other in range(col_count):
                slot = mirrored(place, group_bits) * col_count + other
                item = pltpu.make_async_copy(
                    here.at[chunk, place, pl.ds(other * SUB, SUB)],
                    out.at[pl.ds(slot * local + chunk * SUB, SUB)],
                    out_sems.at[chunk * row_count + place * col_count + other],
                )
                item.start()
                outs.append(item)

    system[...] = jnp.zeros_like(system)

    row_chains, gram_chains = {chunk: [] for chunk in range(chunks)}, []
    pieces = {chunk: [] for chunk in range(chunks)}
    sum_count, gram_count = [0], [0]

    def sum_rows(chunk, first, last):
        columns = pl.ds(first * width, (last - first) * width)
        chain, state = halving(
            projection.at[chunk, :, columns], landing.at[chunk, :, columns], sum_sems,
            sum_count[0] * row_bits,
        )
        sum_count[0] += 1
        pieces[chunk].append((columns, state))
        row_chains[chunk].append(chain)
        return chain

    def sum_gram(number):
        first, size = bounds[number]
        piece = size // row_count
        place = mirrored(row, row_bits) * piece
        target = gram.at[pl.ds(first, size)]
        base = gram_count[0] * 2 * row_bits
        gram_count[0] += 1
        chain, state = halving(
            partial.at[pl.ds(first, size)], gram_landing.at[pl.ds(first, size)], gram_sems, base
        )

        def put():
            target[pl.ds(pl.multiple_of(place, SUB), piece), :] = state["now"][...]

        strides = [1 << i for i in range(row_bits - 1, -1, -1)]
        later = doubling(
            strides, target, gram_sems, base + row_bits, pl.multiple_of(place, SUB), piece
        )
        begin, end = later[0]

        def put_and_begin():
            put()
            begin()

        chain.steps += [(put_and_begin, end)] + later[1:]
        gram_chains.append(chain)
        return chain

    def gather(chunk):
        chain = spread(chunk)
        begin, end = chain.steps[0]

        def join_and_begin():
            for columns, state in pieces[chunk]:
                solved[chunk, :, columns] = state["now"][...]
            begin()

        chain.steps[0] = (join_and_begin, end)
        return chain

    per = len(steps)
    late = chunks - 1
    due = [((number + 1) / len(sends), 2, number) for number in range(len(sends) - per)]
    due += [(0.04 + 0.124 * (i + 1) * 6 / count, 1, panel) for i, panel in enumerate(order)]
    groups = batches(count)
    closing = {panels[-1]: number for number, panels in enumerate(groups) if panels}
    chains, taken, started = [], [], {}
    for time, kind, number in sorted(due):
        for chain in chains:
            chain.tick_at(time)
        if kind == 2:
            arrive(number)
            if (number + 1) % per == 0:
                chunk = number // per
                take_rows(chunk)
                taken.append(chunk)
                started[chunk] = count
        else:
            take_panel(number)
            if number == 0:
                for chunk in taken:
                    send_far(chunk)
            inner(number)
            if number in closing:
                ready = [chunk for chunk in taken if started[chunk] > number]
                for chunk in ready:
                    project(chunk, number, started[chunk])
                fresh = [sum_rows(chunk, number, started[chunk]) for chunk in ready]
                for chunk in ready:
                    started[chunk] = number
                fresh.append(sum_gram(closing[number]))
                for chain in fresh:
                    chain.tick_at(time)
                chains += fresh
    for chunk in range(late):
        if chunk not in far:
            send_far(chunk)
        if started[chunk] > 0:
            project(chunk, 0, started[chunk])
            chain = sum_rows(chunk, 0, started[chunk])
            chain.tick()
            chains.append(chain)
    built = [count]

    def build_ready():
        for number, panels in enumerate(groups):
            if number < len(groups) and not busy(gram_chains[number]):
                lowest = panels[-1] if panels else count - 1
                for panel in range(built[0] - 1, lowest - 1, -1):
                    build(panel)
                    built[0] = panel
            else:
                break

    spreads = {}

    def gather_ready():
        for chunk in range(late):
            if chunk not in spreads and not busy(*row_chains[chunk]):
                spreads[chunk] = gather(chunk)
                spreads[chunk].tick()

    for number in range(AFTER):
        tick(*chains)
    for number in range(late * per, len(sends)):
        arrive(number)
    take_rows(late)
    send_far(late)
    project(late, 0, count)
    final = sum_rows(late, 0, count)
    final.tick()
    while busy(final):
        tick(*chains, *spreads.values())
        gather_ready()
        build_ready()
        final.tick()
    final = gather(late)
    final.tick()
    while busy(*chains) or len(spreads) < late or busy(*spreads.values()):
        tick(*chains, *spreads.values())
        gather_ready()
        build_ready()
        final.tick()
    build_ready()
    finish()
    for chunk in range(late):
        update(chunk)
        final.tick()
    while busy(final):
        final.tick()
    update(late)
    for item in outs:
        item.wait()


def on_device(vectors, reflectors, factors):
    local, total_length = vectors.shape
    row_count = lax.axis_size("row")
    col_count = lax.axis_size("col")
    length = total_length // row_count
    count, part, _ = reflectors.shape
    width = part * col_count
    every = count * width
    chunks = local // SUB
    group = row_count // col_count
    row_bits, group_bits = bits_of(row_count), bits_of(group)
    rows = row_count * SUB
    gram_rows = 0
    for panels in batches(count):
        used = sum((count - 1 - panel) * width for panel in panels)
        gram_rows += padded(used, row_count)
    anywhere = pl.BlockSpec(memory_space=pl.ANY)
    vmem = pl.BlockSpec(memory_space=pltpu.VMEM)
    dma = pltpu.SemaphoreType.DMA
    single, half = jnp.float32, jnp.bfloat16
    return pl.pallas_call(
        functools.partial(kernel, row_count, col_count),
        name="exchange",
        out_shape=jax.ShapeDtypeStruct((local * row_count, length), single),
        in_specs=[anywhere, anywhere, vmem],
        out_specs=anywhere,
        scratch_shapes=[
            pltpu.VMEM((chunks, group, col_count * SUB, length), single),
            pltpu.VMEM((chunks, group, col_count * SUB, length), single),
            pltpu.VMEM((every, length), single),
            pltpu.VMEM((2 * every, length), half),
            pltpu.VMEM((chunks, 2 * rows, length), half),
            pltpu.VMEM((chunks, rows, every), single),
            pltpu.VMEM((chunks, rows, every), single),
            pltpu.VMEM((chunks, group, col_count * SUB, every), single),
            pltpu.VMEM((chunks, SUB, every), single),
            pltpu.VMEM((2 * rows, 2 * every), half),
            pltpu.VMEM((every, every), single),
            pltpu.VMEM((2 * every, every), half),
            pltpu.VMEM((gram_rows, width), single),
            pltpu.VMEM((gram_rows, width), single),
            pltpu.VMEM((gram_rows, width), single),
            dma((2, chunks * row_count)),
            dma((count + chunks,)),
            dma((2, (col_count - 1) * count)),
            dma((2, chunks * col_count)),
            dma((2, 3 * chunks * row_bits)),
            dma((2, chunks * col_count)),
            dma((2, chunks * max(group_bits, 1))),
            dma((2, 3 * 2 * row_bits)),
            dma((chunks * row_count,)),
        ],
        compiler_params=pltpu.CompilerParams(
            collective_id=0, has_side_effects=True, vmem_limit_bytes=60 * 1024 * 1024
        ),
    )(vectors, reflectors, factors)


def solution(mesh):
    return jax.shard_map(
        on_device,
        mesh=mesh,
        in_specs=(P(("row", "col"), None), P(None, "col", "row"), P()),
        out_specs=P("col", "row"),
        check_vma=False,
    )
```

```python
import functools

import jax
import jax.numpy as jnp
from jax import lax
from jax.experimental import pallas as pl
from jax.experimental.pallas import tpu as pltpu
from jax.sharding import PartitionSpec as P

MESH = pl.DeviceIdType.MESH
HIGHEST = lax.Precision.HIGHEST
SUB = 8
WIDER = -5
GAP0 = 0.025
GAP = 0.12
TURNED = (1,)
GRAM_TURNED = ()


def nt(left, right, precision=None):
    return lax.dot_general(
        left,
        right,
        (((1,), (1,)), ((), ())),
        precision=precision,
        preferred_element_type=jnp.float32,
    )


def nn(left, right, precision=None):
    return jnp.dot(left, right, precision=precision, preferred_element_type=jnp.float32)


def split(value):
    top = value.astype(jnp.bfloat16)
    return top, (value - top.astype(jnp.float32)).astype(jnp.bfloat16)


def doubled(value, width):
    columns = value.shape[1]
    pieces = []
    for part in split(value):
        twice = []
        for start in range(0, columns, width):
            piece = part[:, start : start + width]
            twice += [piece, piece]
        pieces.append(jnp.concatenate(twice, axis=1))
    return jnp.concatenate(pieces, axis=0)


def bits_of(count):
    return count.bit_length() - 1


def bit(value, stride):
    return (value // stride) % 2


def mirrored(value, bits):
    found = 0
    for i in range(bits):
        found = found + bit(value, 1 << i) * (1 << (bits - 1 - i))
    return found


def batches(count):
    found = [list(range(count - 2, 1, -1)), [1], [0]]
    return [[panel for panel in panels if panel < count - 1] for panels in found if panels]


def padded(size, row_count):
    unit = SUB * row_count
    return -(-size // unit) * unit


def strides_of(count, turned):
    found = [1 << i for i in range(bits_of(count))]
    return found[:1] + found[2:] + found[1:2] if turned else found


def placed(value, strides):
    found = 0
    for stride in strides:
        found = found * 2 + bit(value, stride)
    return found


def slot_of(place, strides):
    found = 0
    for i, stride in enumerate(reversed(strides)):
        found += bit(place, 1 << i) * stride
    return found


class Chain:
    def __init__(self, steps):
        self.steps = list(steps)
        self.open = None
        self.due = 0.0
        self.made = 0

    def tick_at(self, time):
        if time >= self.due:
            self.tick()
            self.due = time + (GAP0 if self.made == 0 else GAP)
            self.made += 1

    def tick(self):
        if self.open is not None:
            self.open()
            self.open = None
        if self.steps:
            start, end = self.steps.pop(0)
            start()
            self.open = end


def tick(*chains):
    for chain in chains:
        chain.tick()


def busy(*chains):
    return any(chain.open is not None or chain.steps for chain in chains)


def kernel(
    row_count, col_count, vectors, reflectors, factors, out,
    stage, here, held, both, mixed, projection, landing, wide, solved, weights,
    system, pairs, partial, gram_landing, gram,
    row_sems, local_sems, gather_sems, far_sems, sum_sems, cross_sems, wide_sems,
    gram_sems, out_sems,
):
    row = lax.axis_index("row")
    col = lax.axis_index("col")
    chunks = stage.shape[0]
    local = chunks * SUB
    length = held.shape[1]
    count, part, _ = reflectors.shape
    width = part * col_count
    group = row_count // col_count
    row_bits, col_bits, group_bits = bits_of(row_count), bits_of(col_count), bits_of(group)
    rows = row_count * SUB
    high, low = row // group, row % group
    lows = [strides_of(group, chunk in TURNED) for chunk in range(chunks)]
    my_place = [placed(low, strides) for strides in lows]
    highs = [group << i for i in range(col_bits)]

    barrier = pltpu.get_barrier_semaphore()
    for step in range(1, row_count):
        pl.semaphore_signal(
            barrier, inc=1, device_id={"row": lax.rem(row + step, row_count)}, device_id_type=MESH
        )
    for step in range(1, col_count):
        pl.semaphore_signal(
            barrier, inc=1, device_id={"col": lax.rem(col + step, col_count)}, device_id_type=MESH
        )
    pairing = [
        (dh, dc) for dh in range(1, col_count) for dc in range(1, col_count)
    ]
    for dh, dc in pairing:
        pl.semaphore_signal(
            barrier,
            inc=1,
            device_id={
                "row": lax.rem(high + dh, col_count) * group + low,
                "col": lax.rem(col + dc, col_count),
            },
            device_id_type=MESH,
        )
    pl.semaphore_wait(barrier, row_count + col_count - 2 + len(pairing))

    def remote(source, target, sems, number, device, arrival=None):
        return pltpu.make_async_remote_copy(
            src_ref=source,
            dst_ref=target,
            send_sem=sems.at[0, number],
            recv_sem=sems.at[1, number if arrival is None else arrival],
            device_id=device,
            device_id_type=MESH,
        )

    order = list(range(count - 1, -1, -1))
    gathers = {}
    for panel in order:
        place = held.at[pl.ds(pl.multiple_of(panel * width + col * part, SUB), part)]
        gathers[panel] = []
        for step in range(1, col_count):
            item = remote(
                reflectors.at[panel], place, gather_sems, (step - 1) * count + panel,
                {"col": lax.rem(col + step, col_count)},
            )
            item.start()
            gathers[panel].append(item)
    for panel in order:
        place = held.at[pl.ds(pl.multiple_of(panel * width + col * part, SUB), part)]
        item = pltpu.make_async_copy(reflectors.at[panel], place, local_sems.at[panel])
        item.start()
        gathers[panel].append(item)

    middle = row_count // 2
    ranked = sorted(range(1, row_count), key=lambda step: (abs(step - middle), step))
    steps = []
    while ranked:
        steps.append(ranked.pop(0))
        if ranked:
            steps.append(ranked.pop())
    spot = pl.ds(pl.multiple_of(mirrored(high, col_bits) * SUB, SUB), SUB)
    places = [stage.at[chunk, my_place[chunk], spot] for chunk in range(chunks)]
    sends = []
    for chunk in range(chunks):
        for step in steps:
            other = lax.rem(row + step, row_count)
            item = remote(
                vectors.at[
                    pl.ds(chunk * SUB, SUB), pl.ds(pl.multiple_of(other * length, 128), length)
                ],
                places[chunk], row_sems, chunk * row_count + step, {"row": other},
            )
            sends.append(item)
    own_rows = []
    for chunk in range(chunks):
        item = pltpu.make_async_copy(
            vectors.at[
                pl.ds(chunk * SUB, SUB), pl.ds(pl.multiple_of(row * length, 128), length)
            ],
            places[chunk], local_sems.at[count + chunk],
        )
        item.start()
        own_rows.append(item)
    window = len(steps) + WIDER
    for item in sends[:window]:
        item.start()

    def arrive(number):
        sends[number].wait()
        if number + window < len(sends):
            sends[number + window].start()

    def take_rows(chunk):
        own_rows[chunk].wait()
        own = pl.ds(pl.multiple_of(mirrored(col, col_bits) * SUB, SUB), SUB)
        mine = pl.ds(pl.multiple_of(col * SUB, SUB), SUB)
        size = col_count * SUB

        def body(i, carry):
            top, low_part = split(stage[chunk, i])
            at = pl.multiple_of(i * size, size)
            mixed[chunk, pl.ds(at, size), :] = top
            mixed[chunk, pl.ds(pl.multiple_of(rows + at, size), size), :] = low_part
            here[chunk, i, mine, :] = stage[chunk, i, own, :]
            return carry

        lax.fori_loop(0, group, body, 0)

    def take_panel(panel):
        for item in gathers[panel]:
            item.wait()

        def body(i, carry):
            at = pl.multiple_of(panel * width + i * 32, 32)
            top, low_part = split(held[pl.ds(at, 32), :])
            to = pl.multiple_of(2 * panel * width + i * 32, 32)
            both[pl.ds(to, 32), :] = top
            both[pl.ds(pl.multiple_of(to + width, 32), 32), :] = low_part
            return carry

        lax.fori_loop(0, width // 32, body, 0)

    def panel_rows(panel):
        return pl.ds(pl.multiple_of(2 * panel * width, 2 * width), 2 * width)

    def quadrants(value, above, left):
        value = value[:above] + value[above:]
        return value[:, :left] + value[:, left:]

    bases, bounds = {}, []
    base = 0
    for panels in batches(count):
        first = base
        for panel in panels:
            bases[panel] = base
            base += (count - 1 - panel) * width
        used = base
        base = first + padded(used - first, row_count)
        if used < base:
            partial[pl.ds(used, base - used), :] = jnp.zeros((base - used, width), jnp.float32)
        bounds.append((first, base - first))

    def inner(panel):
        def body(i, carry):
            value = nt(both[panel_rows(panel + 1 + i), :], both[panel_rows(panel), :])
            to = pl.multiple_of(bases[panel] + i * width, width)
            partial[pl.ds(to, width), :] = quadrants(value, width, width)
            return carry

        if panel < count - 1:
            lax.fori_loop(0, count - 1 - panel, body, 0)

    def project(chunk, first, last):
        def body(i, carry):
            value = nt(mixed[chunk], both[panel_rows(first + i), :])
            to = pl.ds(pl.multiple_of((first + i) * width, width), width)
            projection[chunk, :, to] = quadrants(value, rows, width)
            return carry

        lax.fori_loop(0, last - first, body, 0)

    def halving(source, target, sems, number, strides):
        total = source.shape[0]
        state = {"now": source}
        steps = []
        for stage_number, stride in enumerate(strides):
            half = total >> (stage_number + 1)
            start = total - (total >> stage_number)

            def begin(stride=stride, half=half, start=start, stage_number=stage_number):
                away = pl.ds(pl.multiple_of((1 - bit(row, stride)) * half, SUB), half)
                place = target.at[pl.ds(start, half)]
                item = remote(
                    state["now"].at[away], place, sems, number + stage_number,
                    {"row": row + stride * (1 - 2 * bit(row, stride))},
                )
                item.start()
                state["item"], state["place"] = item, place

            def end(stride=stride, half=half):
                state["item"].wait()
                keep = pl.ds(pl.multiple_of(bit(row, stride) * half, SUB), half)
                place = state["place"]
                place[...] = place[...] + state["now"][keep, :]
                state["now"] = place

            steps.append((begin, end))
        return Chain(steps), state

    def doubling(strides, target, sems, number, position, size):
        state = {"position": position, "size": size}
        steps = []
        for stage_number, stride in enumerate(strides):
            def begin(stride=stride, stage_number=stage_number):
                where = target.at[pl.ds(state["position"], state["size"])]
                item = remote(
                    where, where, sems, number + stage_number,
                    {"row": row + stride * (1 - 2 * bit(row, stride))},
                )
                item.start()
                state["item"] = item

            def end(stride=stride):
                state["item"].wait()
                state["position"] = state["position"] - bit(row, stride) * state["size"]
                state["size"] = state["size"] * 2

            steps.append((begin, end))
        return steps

    def cross(chunk):
        rows_of = pl.ds(pl.multiple_of(col * SUB, SUB), SUB)
        items = []
        base = chunk * col_count

        def begin():
            place = wide.at[chunk, my_place[chunk], rows_of]
            for step in range(col_count):
                other = lax.rem(high + step, col_count)
                item = remote(
                    solved.at[chunk], place, cross_sems, base + step,
                    {"row": other * group + low, "col": high}, base + col,
                )
                items.append(item)
                if step:
                    item.start()

            @pl.when(col != high)
            def _():
                items[0].start()

            @pl.when(col == high)
            def _():
                wide[chunk, my_place[chunk], rows_of, :] = solved[chunk]

        def end():
            for step in range(1, col_count):
                items[step].wait_send()

            @pl.when(col != high)
            def _():
                items[0].wait_send()

            for other in range(col_count):
                item = remote(
                    solved.at[chunk],
                    wide.at[chunk, my_place[chunk], pl.ds(other * SUB, SUB)],
                    cross_sems, base, {"row": row, "col": col}, base + other,
                )

                @pl.when((col != high) | (col != other))
                def _():
                    item.wait_recv()

        return begin, end

    def spread(chunk):
        number = chunk * max(group_bits, 1)
        return Chain(
            [cross(chunk)]
            + doubling(lows[chunk][::-1], wide.at[chunk], wide_sems, number, my_place[chunk], 1)
        )

    far = {}

    def send_far(chunk):
        items = []
        for step in range(1, col_count):
            other = lax.rem(col + step, col_count)
            source = pl.ds(pl.multiple_of(mirrored(other, col_bits) * SUB, SUB), SUB)
            target = pl.ds(pl.multiple_of(col * SUB, SUB), SUB)
            item = remote(
                stage.at[chunk, :, source], here.at[chunk, :, target],
                far_sems, chunk * col_count + step, {"col": other},
            )
            item.start()
            items.append(item)
        far[chunk] = items

    def build(panel):
        at = pl.ds(panel * width, width)
        system[at, at] = factors[panel].T
        if panel < count - 1:
            below = pl.ds((panel + 1) * width, (count - 1 - panel) * width)
            value = nn(system[below, below], gram[pl.ds(bases[panel], below.size), :], HIGHEST)
            system[below, at] = -nt(value, factors[panel], HIGHEST)

    def finish():
        for panel in range(count):
            top, low_part = split(system[pl.ds(panel * width, width), :])
            pairs[pl.ds(2 * panel * width, width), :] = top
            pairs[pl.ds((2 * panel + 1) * width, width), :] = low_part

    outs = []
    tile = 512 if length % 512 == 0 else length

    def update(chunk):
        for item in far[chunk]:
            item.wait()
        value = nn(doubled(wide[chunk].reshape(rows, count * width), width), pairs[...])
        weights[...] = doubled(value[:rows] + value[rows:], width)

        def body(i, carry):
            at = pl.ds(pl.multiple_of(i * tile, tile), tile)
            value = nn(weights[...], both[:, at])
            value = (value[:rows] + value[rows:]).reshape(group, col_count * SUB, tile)
            here[chunk, :, :, at] = here[chunk, :, :, at] - value
            return carry

        lax.fori_loop(0, length // tile, body, 0)
        for place in range(group):
            for other in range(col_count):
                slot = slot_of(place, lows[chunk]) * col_count + other
                item = pltpu.make_async_copy(
                    here.at[chunk, place, pl.ds(other * SUB, SUB)],
                    out.at[pl.ds(slot * local + chunk * SUB, SUB)],
                    out_sems.at[chunk * row_count + place * col_count + other],
                )
                item.start()
                outs.append(item)

    system[...] = jnp.zeros_like(system)

    row_chains, gram_chains = {chunk: [] for chunk in range(chunks)}, []
    pieces = {chunk: [] for chunk in range(chunks)}
    sum_count, gram_count = [0], [0]

    def sum_rows(chunk, first, last):
        columns = pl.ds(first * width, (last - first) * width)
        chain, state = halving(
            projection.at[chunk, :, columns], landing.at[chunk, :, columns], sum_sems,
            sum_count[0] * row_bits, lows[chunk] + highs,
        )
        sum_count[0] += 1
        pieces[chunk].append((columns, state))
        row_chains[chunk].append(chain)
        return chain

    def sum_gram(number):
        first, size = bounds[number]
        piece = size // row_count
        strides = strides_of(row_count, number in GRAM_TURNED)
        place = placed(row, strides) * piece
        target = gram.at[pl.ds(first, size)]
        base = gram_count[0] * 2 * row_bits
        gram_count[0] += 1
        chain, state = halving(
            partial.at[pl.ds(first, size)], gram_landing.at[pl.ds(first, size)], gram_sems, base,
            strides,
        )

        def put():
            target[pl.ds(pl.multiple_of(place, SUB), piece), :] = state["now"][...]

        later = doubling(
            strides[::-1], target, gram_sems, base + row_bits, pl.multiple_of(place, SUB), piece
        )
        begin, end = later[0]

        def put_and_begin():
            put()
            begin()

        chain.steps += [(put_and_begin, end)] + later[1:]
        gram_chains.append(chain)
        return chain

    def gather(chunk):
        chain = spread(chunk)
        begin, end = chain.steps[0]

        def join_and_begin():
            for columns, state in pieces[chunk]:
                solved[chunk, :, columns] = state["now"][...]
            begin()

        chain.steps[0] = (join_and_begin, end)
        return chain

    per = len(steps)
    late = chunks - 1
    due = [((number + 1) / len(sends), 2, number) for number in range(len(sends))]
    due += [(0.04 + 0.124 * (i + 1) * 6 / count, 1, panel) for i, panel in enumerate(order)]
    groups = batches(count)
    closing = {panels[-1]: number for number, panels in enumerate(groups) if panels}
    chains, taken, started, here_now = [], [], {}, count
    for time, kind, number in sorted(due):
        for chain in chains:
            chain.tick_at(time)
        if kind == 2:
            arrive(number)
            if (number + 1) % per == 0 and number < late * per:
                chunk = number // per
                take_rows(chunk)
                taken.append(chunk)
                started[chunk] = count
                send_far(chunk)
                if here_now < count:
                    project(chunk, here_now, count)
        else:
            take_panel(number)
            here_now = number
            inner(number)
            fresh = [sum_gram(closing[number])] if number in closing else []
            for chunk in taken:
                project(chunk, number, number + 1)
                if number in closing:
                    fresh.append(sum_rows(chunk, number, started[chunk]))
                    started[chunk] = number
            for chain in fresh:
                chain.tick_at(time)
            chains += fresh
    for chunk in range(late):
        if chunk not in far:
            send_far(chunk)
        if started[chunk] > 0:
            chain = sum_rows(chunk, 0, started[chunk])
            chain.tick()
            chains.append(chain)
    built = [count]

    def build_ready():
        for number, panels in enumerate(groups):
            if number < len(groups) and not busy(gram_chains[number]):
                lowest = panels[-1] if panels else count - 1
                for panel in range(built[0] - 1, lowest - 1, -1):
                    build(panel)
                    built[0] = panel
            else:
                break

    spreads = {}

    def gather_ready():
        for chunk in range(late):
            if chunk not in spreads and not busy(*row_chains[chunk]):
                spreads[chunk] = gather(chunk)
                spreads[chunk].tick()
    take_rows(late)
    project(late, 0, count)
    final = sum_rows(late, 0, count)
    final.tick()
    updates = list(range(late))
    finished = []

    def compute():
        if built[0]:
            build_ready()
        elif not finished:
            finish()
            finished.append(True)
        elif updates and updates[0] in spreads and not busy(spreads[updates[0]]):
            update(updates.pop(0))

    for closing_step in range(2):
        while busy(final):
            final.tick()
            if closing_step and late not in far:
                send_far(late)
            tick(*chains, *spreads.values())
            gather_ready()
            compute()
        if closing_step == 0:
            final = gather(late)
    while busy(*chains) or len(spreads) < late or busy(*spreads.values()):
        tick(*chains, *spreads.values())
        gather_ready()
    while updates:
        compute()
    update(late)
    for item in outs:
        item.wait()


def on_device(vectors, reflectors, factors):
    local, total_length = vectors.shape
    row_count = lax.axis_size("row")
    col_count = lax.axis_size("col")
    length = total_length // row_count
    count, part, _ = reflectors.shape
    width = part * col_count
    every = count * width
    chunks = local // SUB
    group = row_count // col_count
    row_bits, group_bits = bits_of(row_count), bits_of(group)
    rows = row_count * SUB
    gram_rows = 0
    for panels in batches(count):
        used = sum((count - 1 - panel) * width for panel in panels)
        gram_rows += padded(used, row_count)
    anywhere = pl.BlockSpec(memory_space=pl.ANY)
    vmem = pl.BlockSpec(memory_space=pltpu.VMEM)
    dma = pltpu.SemaphoreType.DMA
    single, half = jnp.float32, jnp.bfloat16
    return pl.pallas_call(
        functools.partial(kernel, row_count, col_count),
        name="exchange",
        out_shape=jax.ShapeDtypeStruct((local * row_count, length), single),
        in_specs=[anywhere, anywhere, vmem],
        out_specs=anywhere,
        scratch_shapes=[
            pltpu.VMEM((chunks, group, col_count * SUB, length), single),
            pltpu.VMEM((chunks, group, col_count * SUB, length), single),
            pltpu.VMEM((every, length), single),
            pltpu.VMEM((2 * every, length), half),
            pltpu.VMEM((chunks, 2 * rows, length), half),
            pltpu.VMEM((chunks, rows, every), single),
            pltpu.VMEM((chunks, rows, every), single),
            pltpu.VMEM((chunks, group, col_count * SUB, every), single),
            pltpu.VMEM((chunks, SUB, every), single),
            pltpu.VMEM((2 * rows, 2 * every), half),
            pltpu.VMEM((every, every), single),
            pltpu.VMEM((2 * every, every), half),
            pltpu.VMEM((gram_rows, width), single),
            pltpu.VMEM((gram_rows, width), single),
            pltpu.VMEM((gram_rows, width), single),
            dma((2, chunks * row_count)),
            dma((count + chunks,)),
            dma((2, (col_count - 1) * count)),
            dma((2, chunks * col_count)),
            dma((2, 3 * chunks * row_bits)),
            dma((2, chunks * col_count)),
            dma((2, chunks * max(group_bits, 1))),
            dma((2, 3 * 2 * row_bits)),
            dma((chunks * row_count,)),
        ],
        compiler_params=pltpu.CompilerParams(
            collective_id=0, has_side_effects=True, vmem_limit_bytes=60 * 1024 * 1024
        ),
    )(vectors, reflectors, factors)


def solution(mesh):
    return jax.shard_map(
        on_device,
        mesh=mesh,
        in_specs=(P(("row", "col"), None), P(None, "col", "row"), P()),
        out_specs=P("col", "row"),
        check_vma=False,
    )
```

```python
import functools

import jax
import jax.numpy as jnp
from jax import lax
from jax.experimental import pallas as pl
from jax.experimental.pallas import tpu as pltpu
from jax.sharding import PartitionSpec as P

MESH = pl.DeviceIdType.MESH
HIGHEST = lax.Precision.HIGHEST
SUB = 8
WIDER = -3
GAP0 = 0.025
GAP = 0.12
TURNED = (1,)
GRAM_TURNED = ()


def nt(left, right, precision=None):
    return lax.dot_general(
        left,
        right,
        (((1,), (1,)), ((), ())),
        precision=precision,
        preferred_element_type=jnp.float32,
    )


def nn(left, right, precision=None):
    return jnp.dot(left, right, precision=precision, preferred_element_type=jnp.float32)


def split(value):
    top = value.astype(jnp.bfloat16)
    return top, (value - top.astype(jnp.float32)).astype(jnp.bfloat16)


def doubled(value, width):
    columns = value.shape[1]
    pieces = []
    for part in split(value):
        twice = []
        for start in range(0, columns, width):
            piece = part[:, start : start + width]
            twice += [piece, piece]
        pieces.append(jnp.concatenate(twice, axis=1))
    return jnp.concatenate(pieces, axis=0)


def bits_of(count):
    return count.bit_length() - 1


def bit(value, stride):
    return (value // stride) % 2


def mirrored(value, bits):
    found = 0
    for i in range(bits):
        found = found + bit(value, 1 << i) * (1 << (bits - 1 - i))
    return found


def batches(count):
    found = [list(range(count - 2, 1, -1)), [1], [0]]
    return [[panel for panel in panels if panel < count - 1] for panels in found if panels]


def padded(size, row_count):
    unit = SUB * row_count
    return -(-size // unit) * unit


def strides_of(count, turned):
    found = [1 << i for i in range(bits_of(count))]
    return found[:1] + found[2:] + found[1:2] if turned else found


def placed(value, strides):
    found = 0
    for stride in strides:
        found = found * 2 + bit(value, stride)
    return found


def slot_of(place, strides):
    found = 0
    for i, stride in enumerate(reversed(strides)):
        found += bit(place, 1 << i) * stride
    return found


class Chain:
    def __init__(self, steps):
        self.steps = list(steps)
        self.open = None
        self.due = 0.0
        self.made = 0

    def tick_at(self, time):
        if time >= self.due:
            self.tick()
            self.due = time + (GAP0 if self.made == 0 else GAP)
            self.made += 1

    def tick(self):
        if self.open is not None:
            self.open()
            self.open = None
        if self.steps:
            start, end = self.steps.pop(0)
            start()
            self.open = end


def tick(*chains):
    for chain in chains:
        chain.tick()


def busy(*chains):
    return any(chain.open is not None or chain.steps for chain in chains)


def kernel(
    row_count, col_count, vectors, reflectors, factors, out,
    stage, here, held, both, mixed, projection, landing, wide, solved, weights,
    system, pairs, partial, gram_landing, gram,
    row_sems, local_sems, gather_sems, far_sems, sum_sems, cross_sems, wide_sems,
    gram_sems, out_sems,
):
    row = lax.axis_index("row")
    col = lax.axis_index("col")
    chunks = stage.shape[0]
    local = chunks * SUB
    length = held.shape[1]
    count, part, _ = reflectors.shape
    width = part * col_count
    group = row_count // col_count
    row_bits, col_bits, group_bits = bits_of(row_count), bits_of(col_count), bits_of(group)
    rows = row_count * SUB
    high, low = row // group, row % group
    lows = [strides_of(group, chunk in TURNED) for chunk in range(chunks)]
    my_place = [placed(low, strides) for strides in lows]
    highs = [group << i for i in range(col_bits)]

    barrier = pltpu.get_barrier_semaphore()
    for step in range(1, row_count):
        pl.semaphore_signal(
            barrier, inc=1, device_id={"row": lax.rem(row + step, row_count)}, device_id_type=MESH
        )
    for step in range(1, col_count):
        pl.semaphore_signal(
            barrier, inc=1, device_id={"col": lax.rem(col + step, col_count)}, device_id_type=MESH
        )
    pairing = [
        (dh, dc) for dh in range(1, col_count) for dc in range(1, col_count)
    ]
    for dh, dc in pairing:
        pl.semaphore_signal(
            barrier,
            inc=1,
            device_id={
                "row": lax.rem(high + dh, col_count) * group + low,
                "col": lax.rem(col + dc, col_count),
            },
            device_id_type=MESH,
        )
    pl.semaphore_wait(barrier, row_count + col_count - 2 + len(pairing))

    def remote(source, target, sems, number, device, arrival=None):
        return pltpu.make_async_remote_copy(
            src_ref=source,
            dst_ref=target,
            send_sem=sems.at[0, number],
            recv_sem=sems.at[1, number if arrival is None else arrival],
            device_id=device,
            device_id_type=MESH,
        )

    order = list(range(count - 1, -1, -1))
    gathers = {}
    for panel in order:
        place = held.at[pl.ds(pl.multiple_of(panel * width + col * part, SUB), part)]
        gathers[panel] = []
        for step in range(1, col_count):
            item = remote(
                reflectors.at[panel], place, gather_sems, (step - 1) * count + panel,
                {"col": lax.rem(col + step, col_count)},
            )
            item.start()
            gathers[panel].append(item)
    for panel in order:
        place = held.at[pl.ds(pl.multiple_of(panel * width + col * part, SUB), part)]
        item = pltpu.make_async_copy(reflectors.at[panel], place, local_sems.at[panel])
        item.start()
        gathers[panel].append(item)

    middle = row_count // 2
    ranked = sorted(range(1, row_count), key=lambda step: (abs(step - middle), step))
    steps = []
    while ranked:
        steps.append(ranked.pop(0))
        if ranked:
            steps.append(ranked.pop())
    spot = pl.ds(pl.multiple_of(mirrored(high, col_bits) * SUB, SUB), SUB)
    places = [stage.at[chunk, my_place[chunk], spot] for chunk in range(chunks)]
    sends = []
    for chunk in range(chunks):
        for step in steps:
            other = lax.rem(row + step, row_count)
            item = remote(
                vectors.at[
                    pl.ds(chunk * SUB, SUB), pl.ds(pl.multiple_of(other * length, 128), length)
                ],
                places[chunk], row_sems, chunk * row_count + step, {"row": other},
            )
            sends.append(item)
    own_rows = []
    for chunk in range(chunks):
        item = pltpu.make_async_copy(
            vectors.at[
                pl.ds(chunk * SUB, SUB), pl.ds(pl.multiple_of(row * length, 128), length)
            ],
            places[chunk], local_sems.at[count + chunk],
        )
        item.start()
        own_rows.append(item)
    window = len(steps) + WIDER
    for item in sends[:window]:
        item.start()

    def arrive(number):
        sends[number].wait()
        if number + window < len(sends):
            sends[number + window].start()

    def take_rows(chunk):
        own_rows[chunk].wait()
        own = pl.ds(pl.multiple_of(mirrored(col, col_bits) * SUB, SUB), SUB)
        mine = pl.ds(pl.multiple_of(col * SUB, SUB), SUB)
        size = col_count * SUB

        def body(i, carry):
            top, low_part = split(stage[chunk, i])
            at = pl.multiple_of(i * size, size)
            mixed[chunk, pl.ds(at, size), :] = top
            mixed[chunk, pl.ds(pl.multiple_of(rows + at, size), size), :] = low_part
            here[chunk, i, mine, :] = stage[chunk, i, own, :]
            return carry

        lax.fori_loop(0, group, body, 0)

    def take_panel(panel):
        for item in gathers[panel]:
            item.wait()

        def body(i, carry):
            at = pl.multiple_of(panel * width + i * 32, 32)
            top, low_part = split(held[pl.ds(at, 32), :])
            to = pl.multiple_of(2 * panel * width + i * 32, 32)
            both[pl.ds(to, 32), :] = top
            both[pl.ds(pl.multiple_of(to + width, 32), 32), :] = low_part
            return carry

        lax.fori_loop(0, width // 32, body, 0)

    def panel_rows(panel):
        return pl.ds(pl.multiple_of(2 * panel * width, 2 * width), 2 * width)

    def quadrants(value, above, left):
        value = value[:above] + value[above:]
        return value[:, :left] + value[:, left:]

    bases, bounds = {}, []
    base = 0
    for panels in batches(count):
        first = base
        for panel in panels:
            bases[panel] = base
            base += (count - 1 - panel) * width
        used = base
        base = first + padded(used - first, row_count)
        if used < base:
            partial[pl.ds(used, base - used), :] = jnp.zeros((base - used, width), jnp.float32)
        bounds.append((first, base - first))

    def inner(panel):
        def body(i, carry):
            value = nt(both[panel_rows(panel + 1 + i), :], both[panel_rows(panel), :])
            to = pl.multiple_of(bases[panel] + i * width, width)
            partial[pl.ds(to, width), :] = quadrants(value, width, width)
            return carry

        if panel < count - 1:
            lax.fori_loop(0, count - 1 - panel, body, 0)

    def project(chunk, first, last):
        def body(i, carry):
            value = nt(mixed[chunk], both[panel_rows(first + i), :])
            to = pl.ds(pl.multiple_of((first + i) * width, width), width)
            projection[chunk, :, to] = quadrants(value, rows, width)
            return carry

        lax.fori_loop(0, last - first, body, 0)

    def halving(source, target, sems, number, strides):
        total = source.shape[0]
        state = {"now": source}
        steps = []
        for stage_number, stride in enumerate(strides):
            half = total >> (stage_number + 1)
            start = total - (total >> stage_number)

            def begin(stride=stride, half=half, start=start, stage_number=stage_number):
                away = pl.ds(pl.multiple_of((1 - bit(row, stride)) * half, SUB), half)
                place = target.at[pl.ds(start, half)]
                item = remote(
                    state["now"].at[away], place, sems, number + stage_number,
                    {"row": row + stride * (1 - 2 * bit(row, stride))},
                )
                item.start()
                state["item"], state["place"] = item, place

            def end(stride=stride, half=half):
                state["item"].wait()
                keep = pl.ds(pl.multiple_of(bit(row, stride) * half, SUB), half)
                place = state["place"]
                place[...] = place[...] + state["now"][keep, :]
                state["now"] = place

            steps.append((begin, end))
        return Chain(steps), state

    def doubling(strides, target, sems, number, position, size):
        state = {"position": position, "size": size}
        steps = []
        for stage_number, stride in enumerate(strides):
            def begin(stride=stride, stage_number=stage_number):
                where = target.at[pl.ds(state["position"], state["size"])]
                item = remote(
                    where, where, sems, number + stage_number,
                    {"row": row + stride * (1 - 2 * bit(row, stride))},
                )
                item.start()
                state["item"] = item

            def end(stride=stride):
                state["item"].wait()
                state["position"] = state["position"] - bit(row, stride) * state["size"]
                state["size"] = state["size"] * 2

            steps.append((begin, end))
        return steps

    def cross(chunk):
        rows_of = pl.ds(pl.multiple_of(col * SUB, SUB), SUB)
        items = []
        base = chunk * col_count

        def begin():
            place = wide.at[chunk, my_place[chunk], rows_of]
            for step in range(col_count):
                other = lax.rem(high + step, col_count)
                item = remote(
                    solved.at[chunk], place, cross_sems, base + step,
                    {"row": other * group + low, "col": high}, base + col,
                )
                items.append(item)
                if step:
                    item.start()

            @pl.when(col != high)
            def _():
                items[0].start()

            @pl.when(col == high)
            def _():
                wide[chunk, my_place[chunk], rows_of, :] = solved[chunk]

        def end():
            for step in range(1, col_count):
                items[step].wait_send()

            @pl.when(col != high)
            def _():
                items[0].wait_send()

            for other in range(col_count):
                item = remote(
                    solved.at[chunk],
                    wide.at[chunk, my_place[chunk], pl.ds(other * SUB, SUB)],
                    cross_sems, base, {"row": row, "col": col}, base + other,
                )

                @pl.when((col != high) | (col != other))
                def _():
                    item.wait_recv()

        return begin, end

    def spread(chunk):
        number = chunk * max(group_bits, 1)
        return Chain(
            [cross(chunk)]
            + doubling(lows[chunk][::-1], wide.at[chunk], wide_sems, number, my_place[chunk], 1)
        )

    far = {}

    def send_far(chunk):
        items = []
        for step in range(1, col_count):
            other = lax.rem(col + step, col_count)
            source = pl.ds(pl.multiple_of(mirrored(other, col_bits) * SUB, SUB), SUB)
            target = pl.ds(pl.multiple_of(col * SUB, SUB), SUB)
            item = remote(
                stage.at[chunk, :, source], here.at[chunk, :, target],
                far_sems, chunk * col_count + step, {"col": other},
            )
            item.start()
            items.append(item)
        far[chunk] = items

    def build(panel):
        at = pl.ds(panel * width, width)
        system[at, at] = factors[panel].T
        if panel < count - 1:
            below = pl.ds((panel + 1) * width, (count - 1 - panel) * width)
            value = nn(system[below, below], gram[pl.ds(bases[panel], below.size), :], HIGHEST)
            system[below, at] = -nt(value, factors[panel], HIGHEST)

    def finish():
        for panel in range(count):
            top, low_part = split(system[pl.ds(panel * width, width), :])
            pairs[pl.ds(2 * panel * width, width), :] = top
            pairs[pl.ds((2 * panel + 1) * width, width), :] = low_part

    outs = []
    tile = 1024 if length % 1024 == 0 else length

    def update(chunk):
        for item in far[chunk]:
            item.wait()
        value = nn(doubled(wide[chunk].reshape(rows, count * width), width), pairs[...])
        weights[...] = doubled(value[:rows] + value[rows:], width)

        def body(i, carry):
            at = pl.ds(pl.multiple_of(i * tile, tile), tile)
            value = nn(weights[...], both[:, at])
            value = (value[:rows] + value[rows:]).reshape(group, col_count * SUB, tile)
            here[chunk, :, :, at] = here[chunk, :, :, at] - value
            return carry

        lax.fori_loop(0, length // tile, body, 0)
        for place in range(group):
            for other in range(col_count):
                slot = slot_of(place, lows[chunk]) * col_count + other
                item = pltpu.make_async_copy(
                    here.at[chunk, place, pl.ds(other * SUB, SUB)],
                    out.at[pl.ds(slot * local + chunk * SUB, SUB)],
                    out_sems.at[chunk * row_count + place * col_count + other],
                )
                item.start()
                outs.append(item)

    system[...] = jnp.zeros_like(system)

    row_chains, gram_chains = {chunk: [] for chunk in range(chunks)}, []
    pieces = {chunk: [] for chunk in range(chunks)}
    sum_count, gram_count = [0], [0]

    def sum_rows(chunk, first, last):
        columns = pl.ds(first * width, (last - first) * width)
        chain, state = halving(
            projection.at[chunk, :, columns], landing.at[chunk, :, columns], sum_sems,
            sum_count[0] * row_bits, lows[chunk] + highs,
        )
        sum_count[0] += 1
        pieces[chunk].append((columns, state))
        row_chains[chunk].append(chain)
        return chain

    def sum_gram(number):
        first, size = bounds[number]
        piece = size // row_count
        strides = strides_of(row_count, number in GRAM_TURNED)
        place = placed(row, strides) * piece
        target = gram.at[pl.ds(first, size)]
        base = gram_count[0] * 2 * row_bits
        gram_count[0] += 1
        chain, state = halving(
            partial.at[pl.ds(first, size)], gram_landing.at[pl.ds(first, size)], gram_sems, base,
            strides,
        )

        def put():
            target[pl.ds(pl.multiple_of(place, SUB), piece), :] = state["now"][...]

        later = doubling(
            strides[::-1], target, gram_sems, base + row_bits, pl.multiple_of(place, SUB), piece
        )
        begin, end = later[0]

        def put_and_begin():
            put()
            begin()

        chain.steps += [(put_and_begin, end)] + later[1:]
        gram_chains.append(chain)
        return chain

    def gather(chunk):
        chain = spread(chunk)
        begin, end = chain.steps[0]

        def join_and_begin():
            for columns, state in pieces[chunk]:
                solved[chunk, :, columns] = state["now"][...]
            begin()

        chain.steps[0] = (join_and_begin, end)
        return chain

    per = len(steps)
    late = chunks - 1
    due = [((number + 1) / len(sends), 2, number) for number in range(len(sends))]
    due += [(0.04 + 0.124 * (i + 1) * 6 / count, 1, panel) for i, panel in enumerate(order)]
    groups = batches(count)
    closing = {panels[-1]: number for number, panels in enumerate(groups) if panels}
    chains, taken, started, here_now = [], [], {}, count
    for time, kind, number in sorted(due):
        for chain in chains:
            chain.tick_at(time)
        if kind == 2:
            arrive(number)
            if (number + 1) % per == 0 and number < late * per:
                chunk = number // per
                take_rows(chunk)
                taken.append(chunk)
                started[chunk] = count
                send_far(chunk)
                if here_now < count:
                    project(chunk, here_now, count)
        else:
            take_panel(number)
            here_now = number
            inner(number)
            fresh = [sum_gram(closing[number])] if number in closing else []
            for chunk in taken:
                project(chunk, number, number + 1)
                if number in closing:
                    fresh.append(sum_rows(chunk, number, started[chunk]))
                    started[chunk] = number
            for chain in fresh:
                chain.tick_at(time)
            chains += fresh
    for chunk in range(late):
        if chunk not in far:
            send_far(chunk)
        if started[chunk] > 0:
            chain = sum_rows(chunk, 0, started[chunk])
            chain.tick()
            chains.append(chain)
    built = [count]

    def build_ready():
        for number, panels in enumerate(groups):
            if number < len(groups) and not busy(gram_chains[number]):
                lowest = panels[-1] if panels else count - 1
                for panel in range(built[0] - 1, lowest - 1, -1):
                    build(panel)
                    built[0] = panel
            else:
                break

    spreads = {}

    def gather_ready():
        for chunk in range(late):
            if chunk not in spreads and not busy(*row_chains[chunk]):
                spreads[chunk] = gather(chunk)
                spreads[chunk].tick()
    take_rows(late)
    project(late, 0, count)
    final = sum_rows(late, 0, count)
    final.tick()
    updates = list(range(late))
    finished = []

    def compute():
        if built[0]:
            build_ready()
        elif not finished:
            finish()
            finished.append(True)
        elif updates and updates[0] in spreads and not busy(spreads[updates[0]]):
            update(updates.pop(0))

    for closing_step in range(2):
        while busy(final):
            final.tick()
            if closing_step and late not in far:
                send_far(late)
            tick(*chains, *spreads.values())
            gather_ready()
            compute()
        if closing_step == 0:
            final = gather(late)
    while busy(*chains) or len(spreads) < late or busy(*spreads.values()):
        tick(*chains, *spreads.values())
        gather_ready()
    while updates:
        compute()
    update(late)
    for item in outs:
        item.wait()


def on_device(vectors, reflectors, factors):
    local, total_length = vectors.shape
    row_count = lax.axis_size("row")
    col_count = lax.axis_size("col")
    length = total_length // row_count
    count, part, _ = reflectors.shape
    width = part * col_count
    every = count * width
    chunks = local // SUB
    group = row_count // col_count
    row_bits, group_bits = bits_of(row_count), bits_of(group)
    rows = row_count * SUB
    gram_rows = 0
    for panels in batches(count):
        used = sum((count - 1 - panel) * width for panel in panels)
        gram_rows += padded(used, row_count)
    anywhere = pl.BlockSpec(memory_space=pl.ANY)
    vmem = pl.BlockSpec(memory_space=pltpu.VMEM)
    dma = pltpu.SemaphoreType.DMA
    single, half = jnp.float32, jnp.bfloat16
    return pl.pallas_call(
        functools.partial(kernel, row_count, col_count),
        name="exchange",
        out_shape=jax.ShapeDtypeStruct((local * row_count, length), single),
        in_specs=[anywhere, anywhere, vmem],
        out_specs=anywhere,
        scratch_shapes=[
            pltpu.VMEM((chunks, group, col_count * SUB, length), single),
            pltpu.VMEM((chunks, group, col_count * SUB, length), single),
            pltpu.VMEM((every, length), single),
            pltpu.VMEM((2 * every, length), half),
            pltpu.VMEM((chunks, 2 * rows, length), half),
            pltpu.VMEM((chunks, rows, every), single),
            pltpu.VMEM((chunks, rows, every), single),
            pltpu.VMEM((chunks, group, col_count * SUB, every), single),
            pltpu.VMEM((chunks, SUB, every), single),
            pltpu.VMEM((2 * rows, 2 * every), half),
            pltpu.VMEM((every, every), single),
            pltpu.VMEM((2 * every, every), half),
            pltpu.VMEM((gram_rows, width), single),
            pltpu.VMEM((gram_rows, width), single),
            pltpu.VMEM((gram_rows, width), single),
            dma((2, chunks * row_count)),
            dma((count + chunks,)),
            dma((2, (col_count - 1) * count)),
            dma((2, chunks * col_count)),
            dma((2, 3 * chunks * row_bits)),
            dma((2, chunks * col_count)),
            dma((2, chunks * max(group_bits, 1))),
            dma((2, 3 * 2 * row_bits)),
            dma((chunks * row_count,)),
        ],
        compiler_params=pltpu.CompilerParams(
            collective_id=0, has_side_effects=True, vmem_limit_bytes=60 * 1024 * 1024
        ),
    )(vectors, reflectors, factors)


def solution(mesh):
    return jax.shard_map(
        on_device,
        mesh=mesh,
        in_specs=(P(("row", "col"), None), P(None, "col", "row"), P()),
        out_specs=P("col", "row"),
        check_vma=False,
    )
```
